32 devices in a mesh: dp: 4 (over y, x), tp: 8 (over z, core).
Axes of the slice: x: 2, y: 2, z: 4, core: 2. Of those that a mesh axis runs over, the one named last changes fastest.
Arguments:
- gradients: bfloat16 [4, 4, 3072, 768], P('dp', None, 'tp'), may hold values from -6 to 6, as said below
- right_factor: float32 [4, 768, 8], replicated, may hold values from -6 to 6
- weights_before: float32 [4, 3072, 768], P(None, 'tp', 'dp'), may hold values from -0.21875 to 0.21875
- momentum: float32 [4, 3072, 768], P(None, 'tp', 'dp'), may hold values from -0.3125 to 0.3125
Outputs:
- new_weights: float32 [4, 3072, 768], P(None, 'tp', 'dp')
- new_basis: float32 [4, 768, 8], replicated
- new_momentum: float32 [4, 3072, 768], P(None, 'tp', 'dp')
The draws below stay inside these ranges and needn't reach their ends.
Inputs may be any that keep to these rules, and one draw needn't show every extreme that they name: gradients holds numbers from -6 to 6.
All inputs are finite; a program needn't handle non-finite values.
Results may differ from the reference program's by a relative error of at most 0.0003.
Values sent between devices are 32-bit elements.
A program may use at most 64 MiB of HBM per device.

```python
import jax
import jax.numpy as jnp
from jax import lax

WIDTH = 768
INNER = 3072
RANK = 8
LAYERS = 4
REPLICAS = 4
N_TP = 8


def draw_gradients(key, part):
    keys = jax.random.split(key, 5)
    level = jnp.exp(jax.random.uniform(keys[4], (1, LAYERS, N_TP, 1, RANK), jnp.float32, -1.3, 1.3))
    left = jax.random.normal(keys[0], (1, LAYERS, N_TP, INNER // N_TP, RANK), jnp.float32) * level
    left = left.reshape(1, LAYERS, INNER, RANK)
    right = jax.random.normal(keys[1], (1, LAYERS, RANK, WIDTH), jnp.float32)
    strength = jax.random.normal(keys[2], (REPLICAS, LAYERS, 1, RANK), jnp.float32)
    noise = jax.random.normal(keys[3], (REPLICAS, LAYERS, INNER, WIDTH), jnp.float32)
    low = jnp.einsum('alir,lrw->aliw', left * strength, right[0])
    values = low * RANK ** (-0.5) + 0.5 * noise
    return jnp.clip(values, -6.0, 6.0).astype(jnp.bfloat16)


def levels(own_key, shape, pieces, smallest, high):
    gain, own = 1.0, jax.random.fold_in(own_key, 6)
    for position, shards_of in pieces:
        steps = jnp.exp(jax.random.uniform(jax.random.fold_in(own, position), (shards_of,), jnp.float32, smallest / len(pieces), high / len(pieces)))
        gain = gain * jnp.repeat(steps, shape[position] // shards_of).reshape([-1 if axis == position else 1 for axis in range(len(shape))])
    return gain


def gaussian(stream_key, shape, spread, bound, cuts=(), held_as=jnp.bfloat16):
    gain = levels(stream_key, shape, cuts, -0.22, 0.18) if cuts else 1.0
    values = jax.random.normal(stream_key, shape, jnp.float32) * spread * gain
    return jnp.minimum(jnp.maximum(values, -bound), bound).astype(held_as)


def setup_inputs(seed: int = 0) -> dict:
    splits = jax.random.split(jax.random.key(seed), 5)
    return {
        "gradients": draw_gradients(jax.random.fold_in(splits[4], 71), 0),
        "right_factor": gaussian(splits[1], (LAYERS, WIDTH, RANK), 1.0, 6.0, (), jnp.float32),
        "weights_before": gaussian(splits[2], (LAYERS, INNER, WIDTH), WIDTH ** -0.5, 0.21875, ((1, 8), (2, 4)), jnp.float32),
        "momentum": gaussian(splits[3], (LAYERS, INNER, WIDTH), 0.05, 0.3125, ((1, 8), (2, 4)), jnp.float32),
    }


def reference(gradients, right_factor, weights_before, momentum):
    small_basis = right_factor.astype(jnp.bfloat16)
    small_basis = lax.optimization_barrier(small_basis)
    left = jnp.einsum('aliw,lwr->lir', gradients.astype(jnp.float32), small_basis.astype(jnp.float32))
    gram = jnp.einsum('lir,lis->lrs', left, left, precision=lax.Precision.HIGHEST)
    gram = gram + 0.001 * lax.optimization_barrier(jnp.mean(jnp.diagonal(gram, axis1=1, axis2=2), axis=1))[:, None, None] * jnp.eye(RANK, dtype=jnp.float32)
    small_left = lax.optimization_barrier(left.astype(jnp.bfloat16))
    right = jnp.einsum('aliw,lir->lwr', gradients.astype(jnp.float32), small_left.astype(jnp.float32))
    root = jnp.linalg.cholesky(gram)
    half = lax.linalg.triangular_solve(root, jnp.swapaxes(right, 1, 2), left_side=True, lower=True)
    mixed = lax.linalg.triangular_solve(root, half, left_side=True, lower=True, transpose_a=True)
    change = jnp.einsum('lir,lrw->liw', left, mixed, precision=lax.Precision.HIGHEST) / REPLICAS
    new_momentum = 0.9 * momentum + change
    new_weights = weights_before - 0.02 * new_momentum
    new_basis = right * lax.rsqrt(lax.optimization_barrier(jnp.mean(right * right, axis=(1, 2), keepdims=True)) + 1e-12)
    return (new_weights, new_basis, new_momentum)
```

```python
import functools

import jax
import jax.numpy as jnp
from jax import lax
from jax.experimental import pallas as pl
from jax.experimental.pallas import tpu as pltpu
from jax.sharding import PartitionSpec as P

MESH = pl.DeviceIdType.MESH
LANES = 128


def split3(x):
    high = x.astype(jnp.bfloat16).astype(jnp.float32)
    rest = x - high
    mid = rest.astype(jnp.bfloat16).astype(jnp.float32)
    low = (rest - mid).astype(jnp.bfloat16).astype(jnp.float32)
    return high, mid, low


def kernel(
    ndp, ntp, grads, basis, weights, momentum,
    out_weights, out_basis, out_momentum,
    g_buf, w_buf, m_buf, lefts, grams, rights, parts, full, y_buf,
    g_sem, wm_sem, left_send, left_recv, gram_send, gram_recv, part_send, part_recv, full_send, full_recv,
):
    layers, rank, rows = lefts.shape[0], lefts.shape[2], lefts.shape[3]
    width = grads.shape[2]
    columns = weights.shape[1]
    n = ndp * ntp
    tiles = width // LANES
    pieces = layers * tiles
    my_dp, my_tp = lax.axis_index("dp"), lax.axis_index("tp")
    me = my_dp * ntp + my_tp

    def device(flat):
        return (flat // ntp, lax.rem(flat, ntp))

    loads = [pltpu.make_async_copy(grads.at[l], g_buf.at[l], g_sem.at[l]) for l in range(layers)]
    for load in loads:
        load.start()
    state_loads = [
        pltpu.make_async_copy(weights, w_buf, wm_sem.at[0]),
        pltpu.make_async_copy(momentum, m_buf, wm_sem.at[1]),
    ]
    for load in state_loads:
        load.start()

    grams[my_tp] = jnp.zeros(grams.shape[1:], jnp.float32)
    barrier = pltpu.get_barrier_semaphore()
    for k in range(1, n):
        pl.semaphore_signal(barrier, inc=1, device_id=device(lax.rem(me + k, n)), device_id_type=MESH)

    def left_copy(l, k):
        return pltpu.make_async_remote_copy(
            src_ref=lefts.at[l, my_dp], dst_ref=lefts.at[l, my_dp],
            send_sem=left_send, recv_sem=left_recv.at[l],
            device_id=(lax.rem(my_dp + k, ndp), my_tp), device_id_type=MESH,
        )

    for l in range(layers):
        loads[l].wait()
        lefts[l, my_dp] = lax.dot_general(
            basis[l], g_buf[l], (((1,), (1,)), ((), ())), preferred_element_type=jnp.float32
        )
        if l == 0:
            pl.semaphore_wait(barrier, n - 1)
        for k in range(1, ndp):
            left_copy(l, k).start()

    def part_copy(j):
        owner = j % n
        return pltpu.make_async_remote_copy(
            src_ref=rights.at[j], dst_ref=parts.at[j // n, me],
            send_sem=part_send, recv_sem=part_recv.at[j // n],
            device_id=(owner // ntp, owner % ntp), device_id_type=MESH,
        )

    all_left = []
    for l in range(layers):
        if ndp > 1:
            landed = lefts.at[l, pl.ds(0, ndp - 1)]
            pltpu.make_async_copy(landed, landed, left_recv.at[l]).wait()
        left = lefts[l, 0]
        for d in range(1, ndp):
            left = left + lefts[l, d]
        all_left.append(left)
        right = jnp.dot(left.astype(jnp.bfloat16), g_buf[l], preferred_element_type=jnp.float32)
        for t in range(tiles):
            rights[l * tiles + t] = right[:, t * LANES:(t + 1) * LANES]
        for t in range(tiles):
            j = l * tiles + t

            @pl.when(me != j % n)
            def _():
                part_copy(j).start()

    stacked = jnp.concatenate(all_left, axis=0)
    products = lax.dot_general(
        stacked, stacked, (((1,), (1,)), ((), ())),
        precision=lax.Precision.HIGHEST, preferred_element_type=jnp.float32,
    )
    where = lax.broadcasted_iota(jnp.int32, (rank, layers * rank), 1) // rank
    packed = jnp.zeros((rank, layers * rank), jnp.float32)
    for l in range(layers):
        packed = jnp.where(where == l, products[l * rank:(l + 1) * rank], packed)
    grams[my_tp, :, :layers * rank] = packed

    def gram_copy(k):
        return pltpu.make_async_remote_copy(
            src_ref=grams.at[my_tp], dst_ref=grams.at[my_tp],
            send_sem=gram_send, recv_sem=gram_recv,
            device_id=(my_dp, lax.rem(my_tp + k, ntp)), device_id_type=MESH,
        )

    for k in range(1, ntp):
        gram_copy(k).start()

    def full_copy(j, k):
        return pltpu.make_async_remote_copy(
            src_ref=full.at[j], dst_ref=full.at[j],
            send_sem=full_send, recv_sem=full_recv.at[j],
            device_id=device(lax.rem(me + k, n)), device_id_type=MESH,
        )

    for j in range(pieces):
        q = j // n

        @pl.when(me == j % n)
        def _():
            landed = parts.at[q, pl.ds(0, n - 1)]
            pltpu.make_async_copy(landed, landed, part_recv.at[q]).wait()
            parts[q, me] = rights[j]
            full[j] = jnp.sum(parts[q], axis=0)
            for k in range(1, n):
                full_copy(j, k).start()

    if ntp > 1:
        landed = grams.at[pl.ds(0, ntp - 1)]
        pltpu.make_async_copy(landed, landed, gram_recv).wait()
    gram_sum = jnp.sum(grams[...], axis=0)
    line = lax.broadcasted_iota(jnp.int32, (rank, rank), 0)
    diagonal = line == lax.broadcasted_iota(jnp.int32, (rank, rank), 1)
    step_line = lax.broadcasted_iota(jnp.int32, (rank, 1), 0)
    systems = []
    for l in range(layers):
        gram = gram_sum[:, l * rank:(l + 1) * rank]
        ridge = 0.001 * (jnp.sum(jnp.where(diagonal, gram, 0.0)) / rank)
        systems.append((gram + jnp.where(diagonal, ridge, 0.0), all_left[l]))
    for k in range(rank):
        after = []
        for gram, y in systems:
            pivot = 1.0 / gram[k:k + 1, k:k + 1]
            gram_row, y_row = gram[k:k + 1] * pivot, y[k:k + 1] * pivot
            factor = gram[:, k:k + 1]
            here = step_line == k
            after.append((
                jnp.where(here, gram_row, gram - factor * gram_row),
                jnp.where(here, y_row, y - factor * y_row),
            ))
        systems = after
    for l in range(layers):
        high, mid, low = split3(systems[l][1])
        y = jnp.concatenate([high, high, high, mid, mid, low], axis=0)
        y_buf[l] = y.astype(jnp.bfloat16)
    for load in state_loads:
        load.wait()

    shift = lax.rem(width - my_dp * columns, width)
    for l in range(layers):
        for t in range(tiles):
            j = l * tiles + t

            @pl.when(me != j % n)
            def _():
                pltpu.make_async_copy(full.at[j], full.at[j], full_recv.at[j]).wait()
        right = jnp.concatenate([full[l * tiles + t] for t in range(tiles)], axis=1)
        own = pltpu.roll(right, shift, 1)[:, :columns]
        high, mid, low = split3(own)
        own = jnp.concatenate([high, mid, low, high, mid, high], axis=0).T.astype(jnp.bfloat16)
        change = jnp.dot(own, y_buf[l], preferred_element_type=jnp.float32) / ndp
        moved = 0.9 * m_buf[l] + change
        out_momentum[l] = moved
        out_weights[l] = w_buf[l] - 0.02 * moved
        out_basis[l] = right * lax.rsqrt(jnp.mean(right * right) + 1e-12)

    for l in range(layers):
        for k in range(1, ndp):
            left_copy(l, k).wait_send()
    for k in range(1, ntp):
        gram_copy(k).wait_send()
    for j in range(pieces):

        @pl.when(me != j % n)
        def _():
            part_copy(j).wait_send()

        @pl.when(me == j % n)
        def _():
            for k in range(1, n):
                full_copy(j, k).wait_send()


def solution(mesh):
    ndp, ntp = mesh.shape["dp"], mesh.shape["tp"]
    n = ndp * ntp

    def on_device(gradients, right_factor, weights_before, momentum):
        layers, rows, width = gradients.shape[1:]
        rank = right_factor.shape[2]
        columns = weights_before.shape[2]
        pieces = layers * (width // LANES)
        rounds = -(-pieces // n)
        basis = jnp.swapaxes(right_factor, 1, 2).astype(jnp.bfloat16)
        f32 = jnp.float32
        keep = functools.partial(pltpu.with_memory_space_constraint, memory_space=pltpu.HBM)
        new_weights, new_basis, new_momentum = pl.pallas_call(
            functools.partial(kernel, ndp, ntp),
            out_shape=(
                jax.ShapeDtypeStruct((layers, columns, rows), f32),
                jax.ShapeDtypeStruct((layers, rank, width), f32),
                jax.ShapeDtypeStruct((layers, columns, rows), f32),
            ),
            in_specs=[
                pl.BlockSpec(memory_space=pltpu.HBM),
                pl.BlockSpec(memory_space=pltpu.VMEM),
                pl.BlockSpec(memory_space=pltpu.HBM),
                pl.BlockSpec(memory_space=pltpu.HBM),
            ],
            out_specs=[pl.BlockSpec(memory_space=pltpu.VMEM)] * 3,
            scratch_shapes=[
                pltpu.VMEM((layers, rows, width), jnp.bfloat16),
                pltpu.VMEM((layers, columns, rows), f32),
                pltpu.VMEM((layers, columns, rows), f32),
                pltpu.VMEM((layers, ndp, rank, rows), f32),
                pltpu.VMEM((ntp, rank, LANES), f32),
                pltpu.VMEM((pieces, rank, LANES), f32),
                pltpu.VMEM((rounds, n, rank, LANES), f32),
                pltpu.VMEM((pieces, rank, LANES), f32),
                pltpu.VMEM((layers, 6 * rank, rows), jnp.bfloat16),
                pltpu.SemaphoreType.DMA((layers,)),
                pltpu.SemaphoreType.DMA((2,)),
                pltpu.SemaphoreType.DMA,
                pltpu.SemaphoreType.DMA((layers,)),
                pltpu.SemaphoreType.DMA,
                pltpu.SemaphoreType.DMA,
                pltpu.SemaphoreType.DMA,
                pltpu.SemaphoreType.DMA((rounds,)),
                pltpu.SemaphoreType.DMA,
                pltpu.SemaphoreType.DMA((pieces,)),
            ],
            compiler_params=pltpu.CompilerParams(
                collective_id=0, has_side_effects=True, vmem_limit_bytes=24 * 1024 * 1024
            ),
        )(
            keep(gradients[0]), basis,
            keep(jnp.swapaxes(weights_before, 1, 2)), keep(jnp.swapaxes(momentum, 1, 2)),
        )
        return tuple(jnp.swapaxes(x, 1, 2) for x in (new_weights, new_basis, new_momentum))

    in_specs = (P("dp", None, "tp", None), P(), P(None, "tp", "dp"), P(None, "tp", "dp"))
    out_specs = (P(None, "tp", "dp"), P(), P(None, "tp", "dp"))
    return jax.shard_map(on_device, mesh=mesh, in_specs=in_specs, out_specs=out_specs, check_vma=False)
```

```python
import functools

import jax
import jax.numpy as jnp
from jax import lax
from jax.experimental import pallas as pl
from jax.experimental.pallas import tpu as pltpu
from jax.sharding import PartitionSpec as P

MESH = pl.DeviceIdType.MESH
LANES = 128


def split3(x):
    high = x.astype(jnp.bfloat16).astype(jnp.float32)
    rest = x - high
    mid = rest.astype(jnp.bfloat16).astype(jnp.float32)
    low = (rest - mid).astype(jnp.bfloat16).astype(jnp.float32)
    return high, mid, low


def kernel(
    ndp, ntp, grads, basis, weights, momentum,
    out_weights, out_basis, out_momentum,
    b_buf, g_buf, w_buf, m_buf, lefts, grams, rights, parts, full, y_buf,
    g_sem, wm_sem, left_send, left_recv, gram_send, gram_recv, part_send, part_recv, full_send, full_recv,
):
    layers, rank, rows = lefts.shape[0], lefts.shape[2], lefts.shape[3]
    width = grads.shape[2]
    columns = weights.shape[1]
    n = ndp * ntp
    tiles = width // LANES
    pieces = layers * tiles
    my_dp, my_tp = lax.axis_index("dp"), lax.axis_index("tp")
    me = my_dp * ntp + my_tp

    group = -(-pieces // ndp)
    span = max(
        ((d + 1) * columns - 1) // LANES - d * columns // LANES + 1 for d in range(ndp)
    )

    def device(flat):
        return (flat // ntp, lax.rem(flat, ntp))

    def owner_of(l, t):
        place = t * layers + l
        within = place % group
        tp = within * ntp // group if group <= ntp else within % ntp
        return place // group * ntp + tp

    def round_of(l, t):
        return 0 if group <= ntp else (t * layers + l) % group // ntp

    def first_tile(d, least=min):
        return least(d * columns // LANES, tiles - span)

    loads = [pltpu.make_async_copy(grads.at[l], g_buf.at[l], g_sem.at[l]) for l in range(layers)]
    for load in loads:
        load.start()
    basis_load = pltpu.make_async_copy(basis, b_buf, wm_sem.at[2])
    basis_load.start()
    state_loads = [
        pltpu.make_async_copy(weights, w_buf, wm_sem.at[0]),
        pltpu.make_async_copy(momentum, m_buf, wm_sem.at[1]),
    ]
    for load in state_loads:
        load.start()

    grams[my_tp] = jnp.zeros(grams.shape[1:], jnp.float32)
    barrier = pltpu.get_barrier_semaphore()
    for k in range(1, n):
        pl.semaphore_signal(barrier, inc=1, device_id=device(lax.rem(me + k, n)), device_id_type=MESH)

    def left_copy(l, k):
        return pltpu.make_async_remote_copy(
            src_ref=lefts.at[l, my_dp], dst_ref=lefts.at[l, my_dp],
            send_sem=left_send, recv_sem=left_recv.at[l],
            device_id=(lax.rem(my_dp + k, ndp), my_tp), device_id_type=MESH,
        )

    for l in range(layers):
        if l == 0:
            basis_load.wait()
        loads[l].wait()
        lefts[l, my_dp] = lax.dot_general(
            b_buf[l].astype(jnp.bfloat16), g_buf[l], (((1,), (1,)), ((), ())), preferred_element_type=jnp.float32
        )
        if l == 0:
            pl.semaphore_wait(barrier, n - 1)
        for k in range(1, ndp):
            left_copy(l, k).start()

    def part_copy(l, t):
        j, owner, turn = l * tiles + t, owner_of(l, t), round_of(l, t)
        return pltpu.make_async_remote_copy(
            src_ref=rights.at[j], dst_ref=parts.at[turn, me],
            send_sem=part_send, recv_sem=part_recv.at[turn],
            device_id=(owner // ntp, owner % ntp), device_id_type=MESH,
        )

    all_left = []
    for l in range(layers):
        if ndp > 1:
            landed = lefts.at[l, pl.ds(0, ndp - 1)]
            pltpu.make_async_copy(landed, landed, left_recv.at[l]).wait()
        left = lefts[l, 0]
        for d in range(1, ndp):
            left = left + lefts[l, d]
        all_left.append(left)
        right = jnp.dot(left.astype(jnp.bfloat16), g_buf[l], preferred_element_type=jnp.float32)
        for t in range(tiles):
            rights[l * tiles + t] = right[:, t * LANES:(t + 1) * LANES]
        for t in range(tiles):

            @pl.when(me != owner_of(l, t))
            def _():
                part_copy(l, t).start()

    stacked = jnp.concatenate(all_left, axis=0)
    products = lax.dot_general(
        stacked, stacked, (((1,), (1,)), ((), ())),
        precision=lax.Precision.HIGHEST, preferred_element_type=jnp.float32,
    )
    where = lax.broadcasted_iota(jnp.int32, (rank, layers * rank), 1) // rank
    packed = jnp.zeros((rank, layers * rank), jnp.float32)
    for l in range(layers):
        packed = jnp.where(where == l, products[l * rank:(l + 1) * rank], packed)
    grams[my_tp, :, :layers * rank] = packed

    def gram_copy(k):
        return pltpu.make_async_remote_copy(
            src_ref=grams.at[my_tp], dst_ref=grams.at[my_tp],
            send_sem=gram_send, recv_sem=gram_recv,
            device_id=(my_dp, lax.rem(my_tp + k, ntp)), device_id_type=MESH,
        )

    for k in range(1, ntp):
        gram_copy(k).start()

    every = [(l, t) for l in range(layers) for t in range(tiles)]

    def full_copies(l, t):
        j, owner = l * tiles + t, owner_of(l, t)
        others = [(d, p) for d in range(ndp) for p in range(ntp) if d * ntp + p != owner]
        others.sort(key=lambda x: (not 0 <= t - first_tile(x[0]) < span, -abs(x[1] - owner % ntp)))
        return [
            pltpu.make_async_remote_copy(
                src_ref=full.at[j], dst_ref=full.at[j],
                send_sem=full_send, recv_sem=full_recv.at[j],
                device_id=other, device_id_type=MESH,
            )
            for other in others
        ]

    for l, t in every:
        q, j = round_of(l, t), l * tiles + t

        @pl.when(me == owner_of(l, t))
        def _():
            landed = parts.at[q, pl.ds(0, n - 1)]
            pltpu.make_async_copy(landed, landed, part_recv.at[q]).wait()
            parts[q, me] = rights[j]
            full[j] = jnp.sum(parts[q], axis=0)
            for copy in full_copies(l, t):
                copy.start()

    if ntp > 1:
        landed = grams.at[pl.ds(0, ntp - 1)]
        pltpu.make_async_copy(landed, landed, gram_recv).wait()
    gram_sum = jnp.sum(grams[...], axis=0)
    line = lax.broadcasted_iota(jnp.int32, (rank, rank), 0)
    diagonal = line == lax.broadcasted_iota(jnp.int32, (rank, rank), 1)
    step_line = lax.broadcasted_iota(jnp.int32, (rank, 1), 0)
    systems = []
    for l in range(layers):
        gram = gram_sum[:, l * rank:(l + 1) * rank]
        ridge = 0.001 * (jnp.sum(jnp.where(diagonal, gram, 0.0)) / rank)
        systems.append((gram + jnp.where(diagonal, ridge, 0.0), all_left[l]))
    for k in range(rank):
        after = []
        for gram, y in systems:
            pivot = 1.0 / gram[k:k + 1, k:k + 1]
            gram_row, y_row = gram[k:k + 1] * pivot, y[k:k + 1] * pivot
            factor = gram[:, k:k + 1]
            here = step_line == k
            after.append((
                jnp.where(here, gram_row, gram - factor * gram_row),
                jnp.where(here, y_row, y - factor * y_row),
            ))
        systems = after
    for l in range(layers):
        high, mid, low = split3(systems[l][1])
        y = jnp.concatenate([high, high, high, mid, mid, low], axis=0)
        y_buf[l] = y.astype(jnp.bfloat16)
    for load in state_loads:
        load.wait()

    def wait_full(j):
        pltpu.make_async_copy(full.at[j], full.at[j], full_recv.at[j]).wait()

    start = first_tile(my_dp, jnp.minimum)
    shift = lax.rem(span * LANES - (my_dp * columns - start * LANES), span * LANES)
    for l in range(layers):
        for i in range(span):
            t = start + i

            @pl.when(me != owner_of(l, t))
            def _():
                wait_full(l * tiles + t)
        near = jnp.concatenate([full[l * tiles + start + i] for i in range(span)], axis=1)
        own = pltpu.roll(near, shift, 1)[:, :columns]
        high, mid, low = split3(own)
        own = jnp.concatenate([high, mid, low, high, mid, high], axis=0).T.astype(jnp.bfloat16)
        change = jnp.dot(own, y_buf[l], preferred_element_type=jnp.float32) / ndp
        moved = 0.9 * m_buf[l] + change
        out_momentum[l] = moved
        out_weights[l] = w_buf[l] - 0.02 * moved

    for l in range(layers):
        for t in range(tiles):

            @pl.when((me != owner_of(l, t)) & ((t < start) | (t >= start + span)))
            def _():
                wait_full(l * tiles + t)
        right = jnp.concatenate([full[l * tiles + t] for t in range(tiles)], axis=1)
        out_basis[l] = right * lax.rsqrt(jnp.mean(right * right) + 1e-12)

    for l in range(layers):
        for k in range(1, ndp):
            left_copy(l, k).wait_send()
    for k in range(1, ntp):
        gram_copy(k).wait_send()
    for l, t in every:

        @pl.when(me != owner_of(l, t))
        def _():
            part_copy(l, t).wait_send()

        @pl.when(me == owner_of(l, t))
        def _():
            for copy in full_copies(l, t):
                copy.wait_send()


def solution(mesh):
    ndp, ntp = mesh.shape["dp"], mesh.shape["tp"]
    n = ndp * ntp

    def on_device(gradients, right_factor, weights_before, momentum):
        layers, rows, width = gradients.shape[1:]
        rank = right_factor.shape[2]
        columns = weights_before.shape[2]
        pieces = layers * (width // LANES)
        rounds = -(-(-(-pieces // ndp)) // ntp)
        basis = jnp.swapaxes(right_factor, 1, 2)
        f32 = jnp.float32
        keep = functools.partial(pltpu.with_memory_space_constraint, memory_space=pltpu.HBM)
        new_weights, new_basis, new_momentum = pl.pallas_call(
            functools.partial(kernel, ndp, ntp),
            out_shape=(
                jax.ShapeDtypeStruct((layers, columns, rows), f32),
                jax.ShapeDtypeStruct((layers, rank, width), f32),
                jax.ShapeDtypeStruct((layers, columns, rows), f32),
            ),
            in_specs=[
                pl.BlockSpec(memory_space=pltpu.HBM),
                pl.BlockSpec(memory_space=pltpu.HBM),
                pl.BlockSpec(memory_space=pltpu.HBM),
                pl.BlockSpec(memory_space=pltpu.HBM),
            ],
            out_specs=[pl.BlockSpec(memory_space=pltpu.VMEM)] * 3,
            scratch_shapes=[
                pltpu.VMEM((layers, rank, width), f32),
                pltpu.VMEM((layers, rows, width), jnp.bfloat16),
                pltpu.VMEM((layers, columns, rows), f32),
                pltpu.VMEM((layers, columns, rows), f32),
                pltpu.VMEM((layers, ndp, rank, rows), f32),
                pltpu.VMEM((ntp, rank, LANES), f32),
                pltpu.VMEM((pieces, rank, LANES), f32),
                pltpu.VMEM((rounds, n, rank, LANES), f32),
                pltpu.VMEM((pieces, rank, LANES), f32),
                pltpu.VMEM((layers, 6 * rank, rows), jnp.bfloat16),
                pltpu.SemaphoreType.DMA((layers,)),
                pltpu.SemaphoreType.DMA((3,)),
                pltpu.SemaphoreType.DMA,
                pltpu.SemaphoreType.DMA((layers,)),
                pltpu.SemaphoreType.DMA,
                pltpu.SemaphoreType.DMA,
                pltpu.SemaphoreType.DMA,
                pltpu.SemaphoreType.DMA((rounds,)),
                pltpu.SemaphoreType.DMA,
                pltpu.SemaphoreType.DMA((pieces,)),
            ],
            compiler_params=pltpu.CompilerParams(
                collective_id=0, has_side_effects=True, vmem_limit_bytes=24 * 1024 * 1024
            ),
        )(
            keep(gradients[0]), keep(basis),
            keep(jnp.swapaxes(weights_before, 1, 2)), keep(jnp.swapaxes(momentum, 1, 2)),
        )
        return tuple(jnp.swapaxes(x, 1, 2) for x in (new_weights, new_basis, new_momentum))

    in_specs = (P("dp", None, "tp", None), P(), P(None, "tp", "dp"), P(None, "tp", "dp"))
    out_specs = (P(None, "tp", "dp"), P(), P(None, "tp", "dp"))
    return jax.shard_map(on_device, mesh=mesh, in_specs=in_specs, out_specs=out_specs, check_vma=False)
```
